32 devices in a mesh: ctx: 8 (over z, x), head: 4 (over y, core).
Axes of the slice: x: 2, y: 2, z: 4, core: 2. Of those that a mesh axis runs over, the one named last changes fastest.
Arguments:
- activations: bfloat16 [8192, 2048], P('ctx', 'head'), may hold values from -6 to 6
- w_query: bfloat16 [2048, 2048], P('ctx', 'head'), may hold values from -0.125 to 0.125
- w_key: bfloat16 [2048, 2048], P('ctx', 'head'), may hold values from -0.125 to 0.125
- w_value: bfloat16 [2048, 2048], P('ctx', 'head'), may hold values from -0.125 to 0.125
- level_table: float32 [16, 64, 14], P('head'), may hold values from 0.2 to 2
- table_rows: int32 [8192], P('ctx'), may hold values from 0 to 63
- out_grad: bfloat16 [8192, 2048], P('ctx', 'head'), may hold values from -0.059814453 to 0.059814453
Outputs:
- attended: bfloat16 [8192, 2048], P('ctx', 'head')
- grad_query: float32 [2048, 2048], P('ctx', 'head')
- grad_key: float32 [2048, 2048], P('ctx', 'head')
- grad_value: float32 [2048, 2048], P('ctx', 'head')
The draws below stay inside these ranges and needn't reach their ends.
All inputs are finite; a program needn't handle non-finite values.
Results may differ from the reference program's by a relative error of at most 0.0056.
Values may be sent and summed in bfloat16 or wider, within the bound.
A program may use at most 64 MiB of HBM per device.

```python
import math
import jax
import jax.numpy as jnp
from jax import lax

D = 2048
HEADS = 16
HEAD_DIM = 128
TABLE = 64
TOK_DEV = 1024
TOKENS = 8192
LEVELS = 14


def plant(entries, stream_key, low, top_value):
    longest = entries.shape.index(max(entries.shape))
    spots = []
    for shift in (0, 1):
        where = [jax.random.randint(jax.random.fold_in(stream_key, axis), (), 0, length) for axis, length in enumerate(entries.shape)]
        where[longest] = (where[longest] + shift) % entries.shape[longest]
        spots.append(tuple(where))
    return entries.at[spots[0]].set(low).at[spots[1]].set(top_value)


def spiked(array, own_key, source, target, parts, factor):
    owner, partner = [(jnp.arange(array.shape[axis_at]) // (array.shape[axis_at] // parts)).reshape([-1 if axis == axis_at else 1 for axis in range(array.ndim)]) for axis_at in (source, target)]
    chosen = jax.random.permutation(own_key, parts)[partner]
    strong = (owner == chosen) | (owner == (partner + parts // 2) % parts)
    return jnp.where(strong, factor * array, array)


def shard_levels(stream_key, extent, split, least, top_value):
    gain = 1.0
    for position, blocks in split:
        heights = jax.random.uniform(jax.random.fold_in(jax.random.fold_in(stream_key, 6), position), (blocks,), jnp.float32, least / len(split), top_value / len(split))
        gain = gain * jnp.repeat(jnp.exp(heights), extent[position] // blocks).reshape((-1,) + (1,) * (len(extent) - 1 - position))
    return gain


def gaussian(stream_key, extent, deviation, reach, shards=(), kind=jnp.bfloat16):
    values = deviation * jax.random.normal(stream_key, extent, jnp.float32)
    if shards:
        values = values * shard_levels(stream_key, extent, shards, -0.22, 0.18)
    return jnp.clip(values, -reach, reach).astype(kind)


def heavy_noise(rng, extent, width, reach, split, heavy, held_as=jnp.bfloat16):
    array = width * jax.random.normal(rng, extent, jnp.float32)
    if split:
        array = array * shard_levels(rng, extent, split, -0.22, 0.18)
    return jnp.clip(spiked(array, jax.random.fold_in(rng, 3), *heavy), -reach, reach).astype(held_as)


def setup_inputs(seed: int = 0) -> dict:
    key_list = jax.random.split(jax.random.key(seed), 8)
    activations = heavy_noise(key_list[0], (TOKENS, D), 1.0, 6.0, ((0, 8), (1, 4)), (0, 1, 8, 2.0))
    w_query = gaussian(key_list[1], (D, HEADS * HEAD_DIM), D ** -0.5, 0.125, ((0, 8), (1, 4)))
    w_key = gaussian(key_list[2], (D, HEADS * HEAD_DIM), D ** -0.5, 0.125, ((0, 8), (1, 4)))
    w_value = gaussian(key_list[3], (D, HEADS * HEAD_DIM), D ** -0.5, 0.125, ((0, 8), (1, 4)))
    level_table = jnp.clip(jnp.exp(math.log(2.0) - 2.3025851 * jax.random.uniform(key_list[4], (HEADS, TABLE, LEVELS), jnp.float32) ** shard_levels(key_list[4], (HEADS, TABLE, LEVELS), ((0, 4),), -0.2, 0.2)), 0.2, 2.0)
    table_rows = plant(jax.random.randint(key_list[5], (TOKENS,), 0, TABLE), jax.random.fold_in(key_list[5], 1), 0, TABLE - 1).astype(jnp.int32)
    out_grad = gaussian(key_list[6], (TOKENS, HEADS * HEAD_DIM), 0.01, 0.059814453, ((0, 8), (1, 4)))
    return {"activations": activations, "w_query": w_query, "w_key": w_key, "w_value": w_value, "level_table": level_table, "table_rows": table_rows, "out_grad": out_grad}


def level_of(distance, bit_total):
    running = jnp.zeros(distance.shape, jnp.int32)
    for bit_num in range(bit_total):
        running = running + (distance >= 1 << bit_num).astype(jnp.int32)
    return running

def reference(activations, w_query, w_key, w_value, level_table, table_rows, out_grad):
    blocks = TOKENS // TOK_DEV
    inner_bits = int(TOK_DEV).bit_length() - 1
    outer_bits = int(blocks).bit_length() - 1
    scale_factor = 1.0 / math.sqrt(HEAD_DIM * TOK_DEV)
    highest = lax.Precision.HIGHEST
    queries = jnp.dot(activations, w_query, preferred_element_type=jnp.float32).astype(jnp.bfloat16)
    keys = jnp.dot(activations, w_key, preferred_element_type=jnp.float32).astype(jnp.bfloat16)
    values = jnp.dot(activations, w_value, preferred_element_type=jnp.float32).astype(jnp.bfloat16)
    onehot = (table_rows[:, None] == jnp.arange(TABLE, dtype=jnp.int32)[None, :]).astype(jnp.float32)
    lam = jnp.einsum('tr,hrl->thl', onehot, level_table, precision=highest)
    block_shape = (blocks, TOK_DEV, HEADS, HEAD_DIM)
    query_blocks = queries.reshape(block_shape)
    key_blocks = keys.reshape(block_shape)
    value_blocks = values.reshape(block_shape)
    grad_blocks = out_grad.reshape(block_shape)
    lam_blocks = lam.reshape(blocks, TOK_DEV, HEADS, LEVELS)
    positions = jnp.arange(TOK_DEV, dtype=jnp.int32)
    pair_level = level_of(jnp.bitwise_xor(positions[:, None], positions[None, :]), inner_bits + 1)
    causal = positions[:, None] >= positions[None, :]

    def near_block(pieces):
        query_here, key_here, value_here, grad_here, lam_here = pieces
        level_mix = jnp.zeros((HEADS, TOK_DEV, TOK_DEV), jnp.float32)
        for level_num in range(inner_bits + 1):
            level_mix = jnp.where(pair_level[None] == level_num, jnp.transpose(lam_here[:, :, level_num])[:, :, None], level_mix)
        level_mix = jnp.where(causal[None], level_mix * scale_factor, 0.0)
        query_wide = query_here.astype(jnp.float32)
        key_wide = key_here.astype(jnp.float32)
        value_wide = value_here.astype(jnp.float32)
        grad_wide = grad_here.astype(jnp.float32)
        scores = jnp.einsum('thd,shd->hts', query_wide, key_wide)
        attn_probs = (level_mix * scores).astype(jnp.bfloat16).astype(jnp.float32)
        near_out = jnp.einsum('hts,she->the', attn_probs, value_wide)
        grad_scores = jnp.einsum('the,she->hts', grad_wide, value_wide)
        grad_mixed = (level_mix * grad_scores).astype(jnp.bfloat16).astype(jnp.float32)
        query_near = jnp.einsum('hts,shd->thd', grad_mixed, key_wide)
        key_near = jnp.einsum('hts,thd->shd', grad_mixed, query_wide)
        value_near = jnp.einsum('hts,the->she', attn_probs, grad_wide)
        return (near_out, query_near, key_near, value_near)
    near_out, query_near, key_near, value_near = lax.map(near_block, (query_blocks, key_blocks, value_blocks, grad_blocks, lam_blocks))
    query_wide = query_blocks.astype(jnp.float32)
    key_wide = key_blocks.astype(jnp.float32)
    value_wide = value_blocks.astype(jnp.float32)
    grad_wide = grad_blocks.astype(jnp.float32)
    local_states = jnp.einsum('bthd,bthe->bhde', key_wide, value_wide)
    peer_index = jnp.arange(blocks, dtype=jnp.int32)
    peer_level = level_of(jnp.bitwise_xor(peer_index[:, None], peer_index[None, :]), outer_bits + 1)
    earlier = peer_index[None, :] < peer_index[:, None]
    far_out = jnp.zeros(block_shape, jnp.float32)
    query_far = jnp.zeros(block_shape, jnp.float32)
    incoming = jnp.zeros((blocks, HEADS, HEAD_DIM, HEAD_DIM), jnp.float32)
    for bit_num in range(outer_bits):
        member = ((peer_level == bit_num + 1) & earlier).astype(jnp.float32)
        level_sum = jnp.einsum('de,ehij->dhij', member, local_states, precision=highest)
        level_state = lax.optimization_barrier(level_sum.astype(jnp.bfloat16)).astype(jnp.float32)
        level_weight = lam_blocks[:, :, :, inner_bits + 1 + bit_num]
        far_out = far_out + scale_factor * level_weight[..., None] * jnp.einsum('bthd,bhde->bthe', query_wide, level_state)
        query_far = query_far + scale_factor * level_weight[..., None] * jnp.einsum('bthe,bhde->bthd', grad_wide, level_state)
        scaled_query = lax.optimization_barrier(((scale_factor * level_weight)[..., None] * query_wide).astype(jnp.bfloat16)).astype(jnp.float32)
        grad_state = jnp.einsum('bthd,bthe->bhde', scaled_query, grad_wide)
        incoming = incoming + jnp.einsum('de,dhij->ehij', member, grad_state, precision=highest)
    back_state = lax.optimization_barrier(incoming.astype(jnp.bfloat16)).astype(jnp.float32)
    key_far = jnp.einsum('bthe,bhde->bthd', value_wide, back_state)
    value_far = jnp.einsum('bthd,bhde->bthe', key_wide, back_state)
    flat = (TOKENS, HEADS * HEAD_DIM)
    attended = (near_out + far_out).astype(jnp.bfloat16).reshape(flat)
    query_total = (query_near + query_far).astype(jnp.bfloat16).reshape(flat)
    key_total = (key_near + key_far).astype(jnp.bfloat16).reshape(flat)
    value_total = (value_near + value_far).astype(jnp.bfloat16).reshape(flat)
    grad_query = jnp.dot(activations.T, query_total, preferred_element_type=jnp.float32)
    grad_key = jnp.dot(activations.T, key_total, preferred_element_type=jnp.float32)
    grad_value = jnp.dot(activations.T, value_total, preferred_element_type=jnp.float32)
    return (attended, grad_query, grad_key, grad_value)
```

```python
import functools
import math

import jax
import jax.numpy as jnp
from jax import lax
from jax.experimental import pallas as pl
from jax.experimental.pallas import tpu as pltpu
from jax.sharding import PartitionSpec as P

F32 = jnp.float32
BF16 = jnp.bfloat16


def mm(a, b, ca, cb):
    return lax.dot_general(a, b, (((ca,), (cb,)), ((), ())), preferred_element_type=F32)


def from_partner(block, axis, apart):
    count = lax.axis_size(axis)
    route = []
    for low in range(count):
        high = low | 1 << apart
        if high != low and high < count:
            route += [(low, high), (high, low)]
    return lax.ppermute(block, axis, route)


def state_kernel(first_far, outer_bits, q_ref, k_ref, v_ref, g_ref, lam_ref, out_ref):
    q = q_ref[...].astype(F32)
    g = g_ref[...]
    out_ref[0, 0] = mm(k_ref[...], v_ref[...], 0, 0)
    for b in range(outer_bits):
        level = first_far + b
        scaled = (lam_ref[0, :, level : level + 1] * q).astype(BF16)
        out_ref[1 + b, 0] = mm(scaled, g, 0, 0)


def near_kernel(tile, inner_bits, q_ref, k_ref, v_ref, g_ref, lam_ref, out_ref, qn_ref, kn_ref, vn_ref):
    rows, width = q_ref.shape
    chunks = rows // tile
    tile_bits = tile.bit_length() - 1
    r = lax.broadcasted_iota(jnp.int32, (tile, tile), 0)
    s = lax.broadcasted_iota(jnp.int32, (tile, tile), 1)
    apart = jnp.where(r >= s, r ^ s, -1)
    spans = inner_bits - tile_bits
    states = []
    grads = {}
    for c in range(chunks):
        at = pl.ds(c * tile, tile)
        q, k, v, g = q_ref[at], k_ref[at], v_ref[at], g_ref[at]
        if spans:
            states.append(mm(k, v, 0, 0))
        for b in range(spans):
            if c >> b & 1:
                level = tile_bits + 1 + b
                scaled = (lam_ref[0, at, level : level + 1] * q.astype(F32)).astype(BF16)
                grads[b, c] = mm(scaled, g, 0, 0)
    for c in range(chunks):
        at = pl.ds(c * tile, tile)
        q, k, v, g = q_ref[at], k_ref[at], v_ref[at], g_ref[at]
        mix = jnp.where(apart >= 0, lam_ref[0, at, 0:1], 0.0)
        for level in range(1, tile_bits + 1):
            mix = jnp.where(apart >= 1 << (level - 1), lam_ref[0, at, level : level + 1], mix)
        probs = (mix * mm(q, k, 1, 1)).astype(BF16)
        mixed = (mix * mm(g, v, 1, 1)).astype(BF16)
        near = mm(probs, v, 1, 0)
        qn = mm(mixed, k, 1, 0)
        kn = mm(mixed, q, 0, 0)
        vn = mm(probs, g, 0, 0)
        back = None
        for b in range(spans):
            sibling = (c >> b) ^ 1
            members = range(sibling << b, (sibling + 1) << b)
            if c >> b & 1:
                level = tile_bits + 1 + b
                state = sum(states[e] for e in members).astype(BF16)
                weight = lam_ref[0, at, level : level + 1]
                near = near + weight * mm(q, state, 1, 0)
                qn = qn + weight * mm(g, state, 1, 1)
            else:
                part = sum(grads[b, e] for e in members)
                back = part if back is None else back + part
        if back is not None:
            back = back.astype(BF16)
            kn = kn + mm(v, back, 1, 1)
            vn = vn + mm(k, back, 1, 0)
        out_ref[at] = near
        qn_ref[at] = qn
        kn_ref[at] = kn
        vn_ref[at] = vn


def far_kernel(first_far, outer_bits, q_ref, k_ref, v_ref, g_ref, lam_ref, st_ref, back_ref,
               near_ref, qn_ref, kn_ref, vn_ref, out_ref, qt_ref, kt_ref, vt_ref):
    q, k, v, g = q_ref[...], k_ref[...], v_ref[...], g_ref[...]
    near = near_ref[...]
    qn = qn_ref[...]
    for b in range(outer_bits):
        level = first_far + b
        weight = lam_ref[0, :, level : level + 1]
        state = st_ref[b, 0]
        near = near + weight * mm(q, state, 1, 0)
        qn = qn + weight * mm(g, state, 1, 1)
    out_ref[...] = near.astype(BF16)
    qt_ref[...] = qn.astype(BF16)
    back = back_ref[0]
    kt_ref[...] = (kn_ref[...] + mm(v, back, 1, 1)).astype(BF16)
    vt_ref[...] = (vn_ref[...] + mm(k, back, 1, 0)).astype(BF16)


def on_device(activations, w_query, w_key, w_value, level_table, table_rows, out_grad):
    features = lax.all_gather(activations, "head", axis=1, tiled=True)
    rows = features.shape[0]
    columns = w_query.shape[1]
    heads, table_size, level_count = level_table.shape
    width = columns // heads
    inner_bits = rows.bit_length() - 1
    outer_bits = lax.axis_size("ctx").bit_length() - 1
    first_far = inner_bits + 1
    tile = min(256, rows)
    my_index = lax.axis_index("ctx")
    scale = 1.0 / math.sqrt(width * rows)
    onehot = (table_rows[:, None] == jnp.arange(table_size, dtype=jnp.int32)[None, :]).astype(F32)
    lam = scale * jnp.einsum("tr,hrl->htl", onehot, level_table, precision=lax.Precision.HIGHEST)

    def project(w):
        whole = lax.all_gather(w, "ctx", axis=0, tiled=True)
        return jnp.dot(features, whole, preferred_element_type=F32).astype(BF16)

    key = project(w_key)
    value = project(w_value)
    query = project(w_query)

    col = pl.BlockSpec((rows, width), lambda h: (0, h))
    lam_spec = pl.BlockSpec((1, rows, level_count), lambda h: (h, 0, 0))
    packed = pl.pallas_call(
        functools.partial(state_kernel, first_far, outer_bits),
        grid=(heads,),
        in_specs=[col] * 4 + [lam_spec],
        out_specs=pl.BlockSpec((1 + outer_bits, 1, width, width), lambda h: (0, h, 0, 0)),
        out_shape=jax.ShapeDtypeStruct((1 + outer_bits, heads, width, width), F32),
        cost_estimate=pl.CostEstimate(
            flops=2 * rows * columns * width * (1 + outer_bits),
            bytes_accessed=8 * rows * columns, transcendentals=0),
    )(query, key, value, out_grad, lam)

    near_parts = pl.pallas_call(
        functools.partial(near_kernel, tile, inner_bits),
        grid=(heads,),
        in_specs=[col] * 4 + [lam_spec],
        out_specs=[col] * 4,
        out_shape=[jax.ShapeDtypeStruct((rows, columns), F32)] * 4,
        cost_estimate=pl.CostEstimate(
            flops=24 * rows * columns * tile,
            bytes_accessed=24 * rows * columns, transcendentals=0),
    )(query, key, value, out_grad, lam)

    block_sum = packed[0]
    pending = packed[1:]
    incoming = jnp.zeros((heads, width, width), F32)
    levels = []
    for b in range(outer_bits):
        sent = jnp.concatenate([block_sum[None], pending[b:]], axis=0).astype(BF16)
        got = from_partner(sent, "ctx", b).astype(F32)
        is_upper = jnp.right_shift(my_index, b) & 1 == 1
        levels.append(jnp.where(is_upper, got[0], 0.0).astype(BF16))
        incoming = incoming + jnp.where(is_upper, 0.0, got[1])
        if b + 1 < outer_bits:
            block_sum = block_sum + got[0]
            pending = jnp.concatenate([pending[: b + 1], pending[b + 1 :] + got[2:]], axis=0)
    states = jnp.stack(levels)
    back = incoming.astype(BF16)

    attended, q_total, k_total, v_total = pl.pallas_call(
        functools.partial(far_kernel, first_far, outer_bits),
        grid=(heads,),
        in_specs=[col] * 4 + [
            lam_spec,
            pl.BlockSpec((outer_bits, 1, width, width), lambda h: (0, h, 0, 0)),
            pl.BlockSpec((1, width, width), lambda h: (h, 0, 0)),
        ] + [col] * 4,
        out_specs=[col] * 4,
        out_shape=[jax.ShapeDtypeStruct((rows, columns), BF16)] * 4,
        cost_estimate=pl.CostEstimate(
            flops=4 * rows * columns * width * (1 + outer_bits),
            bytes_accessed=32 * rows * columns, transcendentals=0),
    )(query, key, value, out_grad, lam, states, back, *near_parts)

    def gradient(total):
        share = mm(features, total, 0, 0).astype(BF16)
        return lax.psum_scatter(share, "ctx", scatter_dimension=0, tiled=True).astype(F32)

    return attended, gradient(q_total), gradient(k_total), gradient(v_total)


def solution(mesh):
    return jax.shard_map(
        on_device,
        mesh=mesh,
        in_specs=(
            P("ctx", "head"),
            P("ctx", "head"),
            P("ctx", "head"),
            P("ctx", "head"),
            P("head", None, None),
            P("ctx"),
            P("ctx", "head"),
        ),
        out_specs=(P("ctx", "head"), P("ctx", "head"), P("ctx", "head"), P("ctx", "head")),
        check_vma=False,
    )
```
